32 devices in a mesh: bump: 4 (over y, core), nx: 2 (over x), ny: 4 (over z).
Axes of the slice: x: 2, y: 2, z: 4, core: 2. Of those that a mesh axis runs over, the one named last changes fastest.
Arguments:
- payoff: float32 [262144], P(('nx', 'ny')), may hold values from -6 to 6
- positions: float32 [262144], P(('nx', 'ny')), may hold values from -20 to 20
- tables: float32 [8, 5, 262144], P('bump', None, ('nx', 'ny')), may hold values from 0.02 to 1, as said below
- offsets: int32 [8, 1024], P(None, ('nx', 'ny')), may hold values from -1 to 1
- vol_curve: float32 [8], replicated, may hold values from 0.5 to 1.2
- bucket: int32 [64], P('bump'), may hold values from 0 to 7
- bump_size: float32 [64], P('bump'), may hold values from 0.1 to 0.4
Outputs:
- bumped_values: float32 [64, 262144], P('bump', ('nx', 'ny'))
- vega: float32 [64], P('bump')
The draws below stay inside these ranges and needn't reach their ends.
Inputs may be any that keep to these rules, and one draw needn't show every extreme that they name: `tables`: component 0 lies in [0.9, 1], components 1 and 3 in [0.1, 0.2], components 2 and 4 in [0.02, 0.06].
All inputs are finite; a program needn't handle non-finite values.
Results may differ from the reference program's by a relative error of at most 0.0003.
Values sent between devices are 32-bit elements; how exact they have to be, the bound alone decides.
A program may use at most 64 MiB of HBM per device.

```python
import math
import jax
import jax.numpy as jnp
from jax import lax

STEPS = 8
BLOCK = 256
NODES = 262144
BUMPS = 64


def draw_tables(key, part):
    lower = jnp.array([0.9, 0.1, 0.02, 0.1, 0.02], jnp.float32)
    upper = jnp.array([1.0, 0.2, 0.06, 0.2, 0.06], jnp.float32)
    unit = jax.random.uniform(key, (STEPS, 5, NODES), jnp.float32)
    return lower[None, :, None] + (upper - lower)[None, :, None] * unit


def draw_positions(key, part):
    ramp = jnp.exp(jnp.log(3.0) * jnp.arange(NODES, dtype=jnp.float32) / NODES)
    noise = jax.random.normal(key, (NODES,), jnp.float32)
    return jnp.clip(noise * ramp, -6.0, 6.0) * 2.0


def set_ends(values, own_key, least, largest):
    place = [jax.random.randint(jax.random.fold_in(own_key, axis), (), 0, length) for axis, length in enumerate(values.shape)]
    main_axis = values.shape.index(max(values.shape))
    next_to = place[:main_axis] + [(place[main_axis] + 1) % values.shape[main_axis]] + place[main_axis + 1:]
    return values.at[tuple(place)].set(least).at[tuple(next_to)].set(largest)


def block_levels(rng, shape, cuts, least, top_value):
    loudness, own = 1.0, jax.random.fold_in(rng, 6)
    for axis_at, parts in cuts:
        steps = jnp.exp(jax.random.uniform(jax.random.fold_in(own, axis_at), (parts,), jnp.float32, least / len(cuts), top_value / len(cuts)))
        loudness = loudness * jnp.repeat(steps, shape[axis_at] // parts).reshape([-1 if axis == axis_at else 1 for axis in range(len(shape))])
    return loudness


def gaussian(rng, dims, deviation, most, pieces=(), kind=jnp.bfloat16):
    gain = block_levels(rng, dims, pieces, -0.22, 0.18) if pieces else 1.0
    values = jax.random.normal(rng, dims, jnp.float32) * deviation * gain
    return jnp.minimum(jnp.maximum(values, -most), most).astype(kind)


def setup_inputs(seed: int = 0) -> dict:
    key_of = jax.random.split(jax.random.key(seed), 8)
    payoff = gaussian(key_of[0], (NODES,), 1.0, 6.0, ((0, 8),), jnp.float32)
    positions = draw_positions(jax.random.fold_in(key_of[7], 71), 0)
    tables = draw_tables(jax.random.fold_in(key_of[7], 71), 0)
    offsets = set_ends(jax.random.randint(key_of[3], (STEPS, NODES // BLOCK), -1, 2), jax.random.fold_in(key_of[3], 1), -1, 1).astype(jnp.int32)
    vol_curve = jnp.clip(jnp.exp(jax.random.uniform(key_of[4], (STEPS,), jnp.float32, math.log(0.5), math.log(1.2))), 0.5, 1.2)
    bucket = set_ends(jax.random.randint(key_of[5], (BUMPS,), 0, STEPS), jax.random.fold_in(key_of[5], 1), 0, STEPS - 1).astype(jnp.int32)
    bump_size = jnp.clip(jnp.exp(math.log(0.4) - 1.3862944 * jax.random.uniform(key_of[6], (BUMPS,), jnp.float32) ** block_levels(key_of[6], (BUMPS,), ((0, 4),), -0.2, 0.2)), 0.1, 0.4)
    return dict(payoff=payoff, positions=positions, tables=tables, offsets=offsets, vol_curve=vol_curve, bucket=bucket, bump_size=bump_size)


def advance(padded, table, branch_nodes, variance):
    count = padded.shape[-1] - 4

    def shifted(shift_by):
        return padded[..., 2 + shift_by:2 + shift_by + count]

    upward = table[1] + variance * table[2]
    downward = table[3] + variance * table[4]
    middle = 1.0 - upward - downward
    low_case = upward * shifted(0) + middle * shifted(-1) + downward * shifted(-2)
    even_case = upward * shifted(1) + middle * shifted(0) + downward * shifted(-1)
    high_case = upward * shifted(2) + middle * shifted(1) + downward * shifted(0)
    mixed = jnp.where(branch_nodes == -1, low_case, jnp.where(branch_nodes == 0, even_case, high_case))
    return table[0] * mixed


def reference(payoff, positions, tables, offsets, vol_curve, bucket, bump_size):
    block_len = NODES // offsets.shape[1]

    def rollback(variance_row):
        values = payoff
        for step in reversed(range(STEPS)):
            padded = jnp.pad(values, 2, mode="wrap")
            branch_nodes = jnp.repeat(offsets[step], block_len)
            values = advance(padded, tables[step], branch_nodes, variance_row[step])
        return values

    base_values = rollback(vol_curve * vol_curve)
    step_ids = jnp.arange(STEPS, dtype=jnp.int32)
    sigma_rows = vol_curve[None, :] + bump_size[:, None] * (bucket[:, None] == step_ids[None, :]).astype(jnp.float32)

    def one_curve(variance_row):
        values = rollback(variance_row)
        return values, jnp.sum(positions * (values - base_values))

    bumped_values, weighted = lax.map(one_curve, sigma_rows * sigma_rows)
    return bumped_values, weighted / bump_size
```

```python
import functools

import jax
import jax.numpy as jnp
from jax import lax
from jax.experimental import pallas as pl
from jax.experimental.pallas import tpu as pltpu
from jax.sharding import PartitionSpec as P

LANES = 128
SUB = 8
MESH = pl.DeviceIdType.MESH


def sweep_kernel(
    dims,
    vol_ref,
    payoff_ref,
    positions_ref,
    offsets_ref,
    tables_ref,
    rows_ref,
    sums_ref,
    tab,
    pay,
    offs,
    kmask,
    state,
    part,
    part2,
    tab_send,
    tab_recv,
    nb_send,
    nb_recv,
    own_sem,
    res_send,
    res_recv,
    ring_send,
    ring_recv,
    grp_send,
    grp_recv,
):
    n, nx, ny, steps, per, block_len = dims
    ring_size = nx * ny
    rows = payoff_ref.shape[0]
    quarter = rows // n
    ext = quarter + 2 * SUB
    me = lax.axis_index("bump")
    ring = lax.axis_index("nx") * ny + lax.axis_index("ny")

    def at(r, q):
        return {"bump": q, "nx": r // ny, "ny": r % ny}

    right = lax.rem(ring + 1, ring_size)
    left = lax.rem(ring + ring_size - 1, ring_size)
    mine = pl.ds(me * per, per)

    def piece(kind, q):
        if kind == 0:
            return q, ring, slice(q * quarter, (q + 1) * quarter), slice(SUB, SUB + quarter)
        if kind == 1:
            source = slice((q + 1) * quarter - 1, (q + 1) * quarter)
            target = (q + 1) % n
            return target, (right if q == n - 1 else ring), source, slice(SUB - 1, SUB)
        source = slice(q * quarter, q * quarter + 1)
        target = (q - 1) % n
        return target, (left if q == 0 else ring), source, slice(SUB + quarter, SUB + quarter + 1)

    def table_copy(kind, q):
        target, at_ring, source, landing = piece(kind, q)
        crosses = (kind == 1 and q == n - 1) or (kind == 2 and q == 0)
        src = tables_ref.at[:, source]
        dst = tab.at[mine, landing, 0:5]
        remote = pltpu.make_async_remote_copy(
            src_ref=src,
            dst_ref=dst,
            send_sem=tab_send.at[kind, q],
            recv_sem=tab_recv.at[kind, me],
            device_id=at(at_ring, target),
            device_id_type=MESH,
        )
        local = pltpu.make_async_copy(src, dst, tab_recv.at[kind, me])
        return target, crosses, remote, local

    for kind in (1, 2, 0):
        for q in range(n):
            target, crosses, remote, local = table_copy(kind, q)
            if crosses:
                remote.start()
            else:
                pl.when(me != target)(remote.start)
                pl.when(me == target)(local.start)

    def neighbour(i, src, dst, to):
        return pltpu.make_async_remote_copy(
            src_ref=src,
            dst_ref=dst,
            send_sem=nb_send.at[i],
            recv_sem=nb_recv.at[i],
            device_id=at(to, me),
            device_id_type=MESH,
        )

    near = [
        neighbour(0, payoff_ref.at[rows - SUB : rows], pay.at[0:SUB], right),
        neighbour(1, payoff_ref.at[0:SUB], pay.at[SUB + rows : SUB + rows + SUB], left),
        neighbour(2, offsets_ref, offs.at[0], right),
        neighbour(3, offsets_ref, offs.at[1], left),
    ]
    for copy in near:
        copy.start()
    own = pltpu.make_async_copy(payoff_ref, pay.at[SUB : SUB + rows], own_sem)
    own.start()
    for copy in near:
        copy.wait()
    own.wait()

    blocks = offsets_ref.shape[1]
    rows_per_block = block_len // LANES
    row_at = lax.broadcasted_iota(jnp.int32, (ext, blocks), 0) + me * quarter
    row_at = row_at + (rows - SUB)
    block_at = row_at // rows_per_block - blocks
    lane_at = lax.broadcasted_iota(jnp.int32, (ext, blocks), 1)
    for s in range(steps):
        def spread(line, shift):
            hit = lane_at == block_at + shift
            return jnp.where(hit, line.astype(jnp.float32), 0.0)

        picked = (
            spread(offsets_ref[s : s + 1, :], 0)
            + spread(offs[0, s : s + 1, :], blocks)
            + spread(offs[1, s : s + 1, :], -blocks)
        )
        branch = jnp.sum(picked, axis=1, keepdims=True)
        kmask[s] = jnp.broadcast_to(branch, (ext, LANES))

    state[0] = pay[pl.ds(pl.multiple_of(me * quarter, SUB), ext), :]
    lane = lax.broadcasted_iota(jnp.int32, (ext, LANES), 1)

    def waits(src):
        for kind in range(3):
            _, _, source, landing = piece(kind, 0)
            dst = tab.at[pl.ds(src * per, per), landing, 0:5]
            pltpu.make_async_copy(tables_ref.at[:, source], dst, tab_recv.at[kind, src]).wait()

    def shifts(x):
        f1 = pltpu.roll(x, LANES - 1, 1)
        f2 = pltpu.roll(x, LANES - 2, 1)
        b1 = pltpu.roll(x, 1, 1)
        b2 = pltpu.roll(x, 2, 1)
        f1 = jnp.where(lane >= LANES - 1, pltpu.roll(f1, ext - 1, 0), f1)
        f2 = jnp.where(lane >= LANES - 2, pltpu.roll(f2, ext - 1, 0), f2)
        b1 = jnp.where(lane < 1, pltpu.roll(b1, 1, 0), b1)
        b2 = jnp.where(lane < 2, pltpu.roll(b2, 1, 0), b2)
        return b2, b1, f1, f2

    for s in reversed(range(steps)):
        if s % per == per - 1:
            waits(s // per)
        w = vol_ref[s] * vol_ref[s]
        discount = tab[s, :, 0, :]
        slope_up = discount * tab[s, :, 2, :]
        slope_down = discount * tab[s, :, 4, :]
        up = discount * tab[s, :, 1, :] + w * slope_up
        down = discount * tab[s, :, 3, :] + w * slope_down
        middle = discount - up - down
        branch = kmask[s]
        low = branch < -0.5
        high = branch > 0.5

        def moved(x):
            b2, b1, f1, f2 = shifts(x)
            above = jnp.where(low, x, jnp.where(high, f2, f1))
            level = jnp.where(low, b1, jnp.where(high, f1, x))
            below = jnp.where(low, b2, jnp.where(high, x, b1))
            return above, level, below

        for g in [0] + list(range(s + 2, steps + 1)):
            above, level, below = moved(state[g])
            state[g] = up * above + middle * level + down * below
            if g == 0:
                state[s + 1] = slope_up * (above - level) + slope_down * (below - level)

    here = pl.ds(pl.multiple_of(me * quarter, SUB), quarter)
    for g in range(steps + 1):
        rows_ref[g, here, :] = state[g, SUB : SUB + quarter, :]
    weights = positions_ref[here, :]
    for s in range(steps):
        part[ring, s : s + 1, :] = jnp.sum(
            weights * state[s + 1, SUB : SUB + quarter, :], axis=0, keepdims=True
        )

    def result(m, d, slot):
        held = pl.ds(pl.multiple_of(jnp.bitwise_xor(me, m) * quarter, SUB), quarter)
        return pltpu.make_async_remote_copy(
            src_ref=rows_ref.at[:, held, :],
            dst_ref=rows_ref.at[:, held, :],
            send_sem=res_send.at[slot],
            recv_sem=res_recv.at[slot],
            device_id=at(ring, jnp.bitwise_xor(me, d)),
            device_id_type=MESH,
        )

    plan = []
    masks = [0]
    d = n // 2
    while d:
        plan += [(m, d) for m in masks]
        masks = masks + [m | d for m in masks]
        d //= 2
    slots = {m | d: i for i, (m, d) in enumerate(plan)}
    copies = [result(m, d, i) for i, (m, d) in enumerate(plan)]
    for i, (m, d) in enumerate(plan):
        if m == 0:
            copies[i].start()

    ring_copies = []
    for i in range(1, ring_size):
        to = lax.rem(ring + i, ring_size)
        ring_copies.append(
            pltpu.make_async_remote_copy(
                src_ref=part.at[ring],
                dst_ref=part.at[ring],
                send_sem=ring_send.at[i],
                recv_sem=ring_recv.at[i],
                device_id=at(to, me),
                device_id_type=MESH,
            )
        )
    for copy in ring_copies:
        copy.start()
    for i, copy in enumerate(ring_copies, 1):
        copy.wait_send()
        src = lax.rem(ring + ring_size - i, ring_size)
        pltpu.make_async_copy(part.at[src], part.at[src], ring_recv.at[i]).wait()
    part2[me] = jnp.sum(part[...], axis=0)
    grp_copies = []
    for i in range(1, n):
        grp_copies.append(
            pltpu.make_async_remote_copy(
                src_ref=part2.at[me],
                dst_ref=part2.at[me],
                send_sem=grp_send.at[i],
                recv_sem=grp_recv.at[i],
                device_id=at(ring, lax.rem(me + i, n)),
                device_id_type=MESH,
            )
        )
    for copy in grp_copies:
        copy.start()

    for i, (m, d) in enumerate(plan):
        if m != 0:
            copies[slots[m]].wait_recv()
            copies[i].start()
    for i, copy in enumerate(grp_copies, 1):
        copy.wait_send()
        src = lax.rem(me + n - i, n)
        pltpu.make_async_copy(part2.at[src], part2.at[src], grp_recv.at[i]).wait()
    sums_ref[...] = jnp.sum(part2[...], axis=0)
    forwarded = {m for m, _ in plan if m}
    for i, (m, d) in enumerate(plan):
        copies[i].wait_send()
        if m | d not in forwarded:
            copies[i].wait_recv()
    for kind in range(3):
        for q in range(n):
            target, crosses, remote, _ = table_copy(kind, q)
            if crosses:
                remote.wait_send()
            else:
                pl.when(me != target)(remote.wait_send)


def spread_kernel(vol_ref, bucket_ref, bump_ref, rows_ref, sums_ref, out_ref, vega_ref):
    curves = bucket_ref.shape[0]
    base = rows_ref[0]
    for b in range(curves):
        s = bucket_ref[b]
        change = bump_ref[b] * (2.0 * vol_ref[s] + bump_ref[b])
        out_ref[b // SUB, :, b % SUB, :] = base + change * rows_ref[s + 1]

    @pl.when(pl.program_id(0) == 0)
    def _():
        lane = lax.broadcasted_iota(jnp.int32, (1, curves), 1)
        total = jnp.zeros((1, curves), jnp.float32)
        for b in range(curves):
            s = bucket_ref[b]
            slope = 2.0 * vol_ref[s] + bump_ref[b]
            weighted = jnp.sum(sums_ref[pl.ds(s, 1), :], axis=1, keepdims=True)
            total = jnp.where(lane == b, slope * weighted, total)
        vega_ref[...] = total


def on_device(n, nx, ny, payoff, positions, tables, offsets, vol_curve, bucket, bump_size):
    steps = vol_curve.shape[0]
    per, comps, nodes = tables.shape
    curves = bucket.shape[0]
    rows = nodes // LANES
    block_len = nodes // offsets.shape[1]
    quarter = rows // n
    ext = quarter + 2 * SUB
    ring = nx * ny
    tiles = tables.reshape(per, comps, rows, LANES).transpose(0, 2, 1, 3)
    dma = pltpu.SemaphoreType.DMA
    vmem = pl.BlockSpec(memory_space=pltpu.VMEM)
    smem = pl.BlockSpec(memory_space=pltpu.SMEM)
    moved, sums = pl.pallas_call(
        functools.partial(sweep_kernel, (n, nx, ny, steps, per, block_len)),
        out_shape=(
            jax.ShapeDtypeStruct((steps + 1, rows, LANES), jnp.float32),
            jax.ShapeDtypeStruct((steps, LANES), jnp.float32),
        ),
        in_specs=[smem, vmem, vmem, vmem, pl.BlockSpec(memory_space=pl.ANY)],
        out_specs=(vmem, vmem),
        scratch_shapes=[
            pltpu.VMEM((steps, ext, SUB, LANES), jnp.float32),
            pltpu.VMEM((rows + 2 * SUB, LANES), jnp.float32),
            pltpu.VMEM((2,) + offsets.shape, jnp.int32),
            pltpu.VMEM((steps, ext, LANES), jnp.float32),
            pltpu.VMEM((steps + 1, ext, LANES), jnp.float32),
            pltpu.VMEM((ring, steps, LANES), jnp.float32),
            pltpu.VMEM((n, steps, LANES), jnp.float32),
            dma((3, n)),
            dma((3, n)),
            dma((4,)),
            dma((4,)),
            dma,
            dma((n - 1,)),
            dma((n - 1,)),
            dma((ring,)),
            dma((ring,)),
            dma((n,)),
            dma((n,)),
        ],
        compiler_params=pltpu.CompilerParams(has_side_effects=True),
        name="sweep",
    )(
        vol_curve,
        payoff.reshape(rows, LANES),
        positions.reshape(rows, LANES),
        offsets,
        tiles,
    )
    grid = n
    groups = curves // SUB
    bumped, vega = pl.pallas_call(
        spread_kernel,
        grid=(grid,),
        out_shape=(
            jax.ShapeDtypeStruct((groups, rows, SUB, LANES), jnp.float32),
            jax.ShapeDtypeStruct((1, curves), jnp.float32),
        ),
        in_specs=[
            smem,
            smem,
            smem,
            pl.BlockSpec((steps + 1, rows // grid, LANES), lambda i: (0, i, 0)),
            pl.BlockSpec((steps, LANES), lambda i: (0, 0)),
        ],
        out_specs=(
            pl.BlockSpec((groups, rows // grid, SUB, LANES), lambda i: (0, i, 0, 0)),
            pl.BlockSpec((1, curves), lambda i: (0, 0)),
        ),
        name="spread",
    )(vol_curve, bucket, bump_size, moved, sums)
    bumped = bumped.transpose(0, 2, 1, 3).reshape(curves, nodes)
    return bumped, vega.reshape(curves)


def solution(mesh):
    shape = dict(mesh.shape)
    in_specs = (
        P(("nx", "ny")),
        P(("nx", "ny")),
        P("bump", None, ("nx", "ny")),
        P(None, ("nx", "ny")),
        P(),
        P("bump"),
        P("bump"),
    )
    out_specs = (P("bump", ("nx", "ny")), P("bump"))
    body = functools.partial(on_device, shape["bump"], shape["nx"], shape["ny"])
    return jax.shard_map(body, mesh=mesh, in_specs=in_specs, out_specs=out_specs, check_vma=False)
```

```python
import functools

import jax
import jax.numpy as jnp
from jax import lax
from jax.experimental import pallas as pl
from jax.experimental.pallas import tpu as pltpu
from jax.sharding import PartitionSpec as P

LANES = 128
SUB = 8
MESH = pl.DeviceIdType.MESH


def sweep_kernel(
    dims,
    vol_ref,
    payoff_ref,
    positions_ref,
    offsets_ref,
    tables_ref,
    rows_ref,
    sums_ref,
    tab,
    pay,
    offs,
    kmask,
    state,
    part,
    part2,
    tab_send,
    tab_recv,
    nb_send,
    nb_recv,
    own_sem,
    res_send,
    res_recv,
    ring_send,
    ring_recv,
    grp_send,
    grp_recv,
):
    n, nx, ny, steps, per, block_len, chunks = dims
    ring_size = nx * ny
    rows = payoff_ref.shape[0]
    quarter = rows // n
    ext = quarter + 2 * SUB
    span = quarter // chunks
    wide = span + 2 * SUB
    me = lax.axis_index("bump")
    ring = lax.axis_index("nx") * ny + lax.axis_index("ny")

    def at(r, q):
        return {"bump": q, "nx": r // ny, "ny": r % ny}

    right = lax.rem(ring + 1, ring_size)
    left = lax.rem(ring + ring_size - 1, ring_size)

    def neighbour(i, src, dst, to):
        return pltpu.make_async_remote_copy(
            src_ref=src,
            dst_ref=dst,
            send_sem=nb_send.at[i],
            recv_sem=nb_recv.at[i],
            device_id=at(to, me),
            device_id_type=MESH,
        )

    near = [
        neighbour(0, payoff_ref.at[rows - SUB : rows], pay.at[0:SUB], right),
        neighbour(1, payoff_ref.at[0:SUB], pay.at[SUB + rows : SUB + rows + SUB], left),
        neighbour(2, offsets_ref, offs.at[0], right),
        neighbour(3, offsets_ref, offs.at[1], left),
    ]
    for copy in near:
        copy.start()

    last = chunks + 1

    def piece(kind, q):
        if kind == 0:
            source = slice((q + 1) * quarter - 1, (q + 1) * quarter)
            target = (q + 1) % n
            return target, (right if q == n - 1 else ring), source, slice(SUB - 1, SUB)
        if kind == last:
            source = slice(q * quarter, q * quarter + 1)
            target = (q - 1) % n
            landing = slice(SUB + quarter, SUB + quarter + 1)
            return target, (left if q == 0 else ring), source, landing
        lo = 0 if kind == 1 else (kind - 1) * span + SUB
        hi = quarter if kind == chunks else kind * span + SUB
        source = slice(q * quarter + lo, q * quarter + hi)
        return q, ring, source, slice(SUB + lo, SUB + hi)

    def table_copy(kind, q):
        target, at_ring, source, landing = piece(kind, q)
        crosses = (kind == 0 and q == n - 1) or (kind == last and q == 0)
        src = tables_ref.at[:, source]
        dst = tab.at[me, :, landing]

        def remote():
            return pltpu.make_async_remote_copy(
                src_ref=src,
                dst_ref=dst,
                send_sem=tab_send.at[kind, q],
                recv_sem=tab_recv.at[kind, me],
                device_id=at(at_ring, target),
                device_id_type=MESH,
            )

        def local():
            return pltpu.make_async_copy(src, dst, tab_recv.at[kind, me])

        return target, crosses, remote, local

    for kind in range(last + 1):
        for q in range(n):
            target, crosses, remote, local = table_copy(kind, q)
            if crosses:
                remote().start()
            else:
                pl.when(me != target)(lambda: remote().start())
                pl.when(me == target)(lambda: local().start())

    own = pltpu.make_async_copy(payoff_ref, pay.at[SUB : SUB + rows], own_sem)
    own.start()
    for copy in near:
        copy.wait()
    own.wait()

    blocks = offsets_ref.shape[1]
    rows_per_block = block_len // LANES
    row_at = lax.broadcasted_iota(jnp.int32, (ext, blocks), 0) + me * quarter
    row_at = row_at + (rows - SUB)
    block_at = row_at // rows_per_block - blocks
    lane_at = lax.broadcasted_iota(jnp.int32, (ext, blocks), 1)
    for s in range(steps):
        def spread(line, shift):
            hit = lane_at == block_at + shift
            return jnp.where(hit, line.astype(jnp.float32), 0.0)

        picked = (
            spread(offsets_ref[s : s + 1, :], 0)
            + spread(offs[0, s : s + 1, :], blocks)
            + spread(offs[1, s : s + 1, :], -blocks)
        )
        branch = jnp.sum(picked, axis=1, keepdims=True)
        kmask[s] = jnp.broadcast_to(branch, (ext, LANES))

    lane = lax.broadcasted_iota(jnp.int32, (wide, LANES), 1)

    def waits(kind, src):
        _, _, source, landing = piece(kind, 0)
        dst = tab.at[src, :, landing]
        pltpu.make_async_copy(tables_ref.at[:, source], dst, tab_recv.at[kind, src]).wait()

    def shifts(x):
        f1 = pltpu.roll(x, LANES - 1, 1)
        f2 = pltpu.roll(x, LANES - 2, 1)
        b1 = pltpu.roll(x, 1, 1)
        b2 = pltpu.roll(x, 2, 1)
        f1 = jnp.where(lane >= LANES - 1, pltpu.roll(f1, wide - 1, 0), f1)
        f2 = jnp.where(lane >= LANES - 2, pltpu.roll(f2, wide - 1, 0), f2)
        b1 = jnp.where(lane < 1, pltpu.roll(b1, 1, 0), b1)
        b2 = jnp.where(lane < 2, pltpu.roll(b2, 1, 0), b2)
        return b2, b1, f1, f2

    def roll_back(h):
        window = slice(h * span, h * span + wide)
        state[0] = pay[pl.ds(pl.multiple_of(me * quarter + h * span, SUB), wide), :]
        for s in reversed(range(steps)):
            src, step = s // per, s % per
            if step == per - 1:
                if h == 0:
                    waits(0, src)
                waits(h + 1, src)
                if h == chunks - 1:
                    waits(last, src)
            w = vol_ref[s] * vol_ref[s]
            discount = tab[src, 0, window, step, :]
            slope_up = discount * tab[src, 2, window, step, :]
            slope_down = discount * tab[src, 4, window, step, :]
            up = discount * tab[src, 1, window, step, :] + w * slope_up
            down = discount * tab[src, 3, window, step, :] + w * slope_down
            middle = discount - up - down
            branch = kmask[s, window]
            low = branch < -0.5
            high = branch > 0.5
            for g in [0] + list(range(s + 2, steps + 1)):
                x = state[g]
                b2, b1, f1, f2 = shifts(x)
                above = jnp.where(low, x, jnp.where(high, f2, f1))
                level = jnp.where(low, b1, jnp.where(high, f1, x))
                below = jnp.where(low, b2, jnp.where(high, x, b1))
                state[g] = up * above + middle * level + down * below
                if g == 0:
                    state[s + 1] = slope_up * (above - level) + slope_down * (below - level)
        here = pl.ds(pl.multiple_of(me * quarter + h * span, SUB), span)
        weights = positions_ref[here, :]
        for g in range(steps + 1):
            center = state[g, SUB : SUB + span, :]
            rows_ref[g, here, :] = center
            if g:
                weighted = jnp.sum(weights * center, axis=0, keepdims=True)
                if h:
                    weighted = weighted + part[ring, g - 1 : g, :]
                part[ring, g - 1 : g, :] = weighted

    def result(m, d, slot, h):
        first = jnp.bitwise_xor(me, m) * quarter + h * span
        held = pl.ds(pl.multiple_of(first, SUB), span)
        return pltpu.make_async_remote_copy(
            src_ref=rows_ref.at[:, held, :],
            dst_ref=rows_ref.at[:, held, :],
            send_sem=res_send.at[slot, h],
            recv_sem=res_recv.at[slot, h],
            device_id=at(ring, jnp.bitwise_xor(me, d)),
            device_id_type=MESH,
        )

    plan = []
    masks = [0]
    d = n // 2
    while d:
        plan += [(m, d) for m in masks]
        masks = masks + [m | d for m in masks]
        d //= 2
    slots = {m | d: i for i, (m, d) in enumerate(plan)}
    landed = set()
    copies = [[result(m, d, i, h) for h in range(chunks)] for i, (m, d) in enumerate(plan)]
    for h in range(chunks):
        roll_back(h)
        for i, (m, d) in enumerate(plan):
            if m == 0:
                copies[i][h].start()

    ring_copies = []
    for i in range(1, ring_size):
        to = lax.rem(ring + i, ring_size)
        ring_copies.append(
            pltpu.make_async_remote_copy(
                src_ref=part.at[ring],
                dst_ref=part.at[ring],
                send_sem=ring_send.at[i],
                recv_sem=ring_recv.at[i],
                device_id=at(to, me),
                device_id_type=MESH,
            )
        )
    for copy in ring_copies:
        copy.start()
    for i, copy in enumerate(ring_copies, 1):
        copy.wait_send()
        src = lax.rem(ring + ring_size - i, ring_size)
        pltpu.make_async_copy(part.at[src], part.at[src], ring_recv.at[i]).wait()
    part2[me] = jnp.sum(part[...], axis=0)
    grp_copies = []
    for i in range(1, n):
        grp_copies.append(
            pltpu.make_async_remote_copy(
                src_ref=part2.at[me],
                dst_ref=part2.at[me],
                send_sem=grp_send.at[i],
                recv_sem=grp_recv.at[i],
                device_id=at(ring, lax.rem(me + i, n)),
                device_id_type=MESH,
            )
        )
    for copy in grp_copies:
        copy.start()

    for h in range(chunks):
        for i, (m, d) in enumerate(plan):
            if m != 0:
                if (m, h) not in landed:
                    landed.add((m, h))
                    copies[slots[m]][h].wait_recv()
                copies[i][h].start()
    for i, copy in enumerate(grp_copies, 1):
        copy.wait_send()
        src = lax.rem(me + n - i, n)
        pltpu.make_async_copy(part2.at[src], part2.at[src], grp_recv.at[i]).wait()
    sums_ref[...] = jnp.sum(part2[...], axis=0)
    for h in range(chunks):
        for i, (m, d) in enumerate(plan):
            copies[i][h].wait_send()
            if (m | d, h) not in landed:
                copies[i][h].wait_recv()
    for kind in range(last + 1):
        for q in range(n):
            target, crosses, remote, _ = table_copy(kind, q)
            if crosses:
                remote().wait_send()
            else:
                pl.when(me != target)(lambda: remote().wait_send())


def spread_kernel(vol_ref, bucket_ref, bump_ref, rows_ref, sums_ref, out_ref, vega_ref):
    curves = bucket_ref.shape[0]
    base = rows_ref[0]
    for b in range(curves):
        s = bucket_ref[b]
        change = bump_ref[b] * (2.0 * vol_ref[s] + bump_ref[b])
        out_ref[b // SUB, :, b % SUB, :] = base + change * rows_ref[s + 1]

    @pl.when(pl.program_id(0) == 0)
    def _():
        lane = lax.broadcasted_iota(jnp.int32, (1, curves), 1)
        total = jnp.zeros((1, curves), jnp.float32)
        for b in range(curves):
            s = bucket_ref[b]
            slope = 2.0 * vol_ref[s] + bump_ref[b]
            weighted = jnp.sum(sums_ref[pl.ds(s, 1), :], axis=1, keepdims=True)
            total = jnp.where(lane == b, slope * weighted, total)
        vega_ref[...] = total


def on_device(n, nx, ny, payoff, positions, tables, offsets, vol_curve, bucket, bump_size):
    steps = vol_curve.shape[0]
    per, comps, nodes = tables.shape
    curves = bucket.shape[0]
    rows = nodes // LANES
    block_len = nodes // offsets.shape[1]
    quarter = rows // n
    ext = quarter + 2 * SUB
    ring = nx * ny
    chunks = 2
    wide = quarter // chunks + 2 * SUB
    tiles = tables.transpose(1, 0, 2).reshape(comps, per, rows, LANES).transpose(0, 2, 1, 3)
    dma = pltpu.SemaphoreType.DMA
    vmem = pl.BlockSpec(memory_space=pltpu.VMEM)
    smem = pl.BlockSpec(memory_space=pltpu.SMEM)
    moved, sums = pl.pallas_call(
        functools.partial(sweep_kernel, (n, nx, ny, steps, per, block_len, chunks)),
        out_shape=(
            jax.ShapeDtypeStruct((steps + 1, rows, LANES), jnp.float32),
            jax.ShapeDtypeStruct((steps, LANES), jnp.float32),
        ),
        in_specs=[smem, vmem, vmem, vmem, pl.BlockSpec(memory_space=pl.ANY)],
        out_specs=(vmem, vmem),
        scratch_shapes=[
            pltpu.VMEM((n, comps, ext, per, LANES), jnp.float32),
            pltpu.VMEM((rows + 2 * SUB, LANES), jnp.float32),
            pltpu.VMEM((2,) + offsets.shape, jnp.int32),
            pltpu.VMEM((steps, ext, LANES), jnp.float32),
            pltpu.VMEM((steps + 1, wide, LANES), jnp.float32),
            pltpu.VMEM((ring, steps, LANES), jnp.float32),
            pltpu.VMEM((n, steps, LANES), jnp.float32),
            dma((chunks + 2, n)),
            dma((chunks + 2, n)),
            dma((4,)),
            dma((4,)),
            dma,
            dma((n - 1, chunks)),
            dma((n - 1, chunks)),
            dma((ring,)),
            dma((ring,)),
            dma((n,)),
            dma((n,)),
        ],
        compiler_params=pltpu.CompilerParams(has_side_effects=True),
        name="sweep",
    )(
        vol_curve,
        payoff.reshape(rows, LANES),
        positions.reshape(rows, LANES),
        offsets,
        tiles,
    )
    grid = n
    groups = curves // SUB
    bumped, vega = pl.pallas_call(
        spread_kernel,
        grid=(grid,),
        out_shape=(
            jax.ShapeDtypeStruct((groups, rows, SUB, LANES), jnp.float32),
            jax.ShapeDtypeStruct((1, curves), jnp.float32),
        ),
        in_specs=[
            smem,
            smem,
            smem,
            pl.BlockSpec((steps + 1, rows // grid, LANES), lambda i: (0, i, 0)),
            pl.BlockSpec((steps, LANES), lambda i: (0, 0)),
        ],
        out_specs=(
            pl.BlockSpec((groups, rows // grid, SUB, LANES), lambda i: (0, i, 0, 0)),
            pl.BlockSpec((1, curves), lambda i: (0, 0)),
        ),
        name="spread",
    )(vol_curve, bucket, bump_size, moved, sums)
    bumped = bumped.transpose(0, 2, 1, 3).reshape(curves, nodes)
    return bumped, vega.reshape(curves)


def solution(mesh):
    shape = dict(mesh.shape)
    in_specs = (
        P(("nx", "ny")),
        P(("nx", "ny")),
        P("bump", None, ("nx", "ny")),
        P(None, ("nx", "ny")),
        P(),
        P("bump"),
        P("bump"),
    )
    out_specs = (P("bump", ("nx", "ny")), P("bump"))
    body = functools.partial(on_device, shape["bump"], shape["nx"], shape["ny"])
    return jax.shard_map(body, mesh=mesh, in_specs=in_specs, out_specs=out_specs, check_vma=False)
```

```python
import functools

import jax
import jax.numpy as jnp
from jax import lax
from jax.experimental import pallas as pl
from jax.experimental.pallas import tpu as pltpu
from jax.sharding import PartitionSpec as P

LANES = 128
SUB = 8
MESH = pl.DeviceIdType.MESH


def sweep_kernel(
    dims,
    vol_ref,
    payoff_ref,
    positions_ref,
    offsets_ref,
    tables_ref,
    rows_ref,
    sums_ref,
    tab,
    pay,
    offs,
    kmask,
    state,
    part,
    part2,
    tab_send,
    tab_recv,
    nb_send,
    nb_recv,
    own_sem,
    res_send,
    res_recv,
    ring_send,
    ring_recv,
    grp_send,
    grp_recv,
):
    n, nx, ny, steps, per, block_len, chunks = dims
    ring_size = nx * ny
    rows = payoff_ref.shape[0]
    quarter = rows // n
    ext = quarter + 2 * SUB
    span = quarter // chunks
    wide = span + 2 * SUB
    me = lax.axis_index("bump")
    ring = lax.axis_index("nx") * ny + lax.axis_index("ny")

    def at(r, q):
        return {"bump": q, "nx": r // ny, "ny": r % ny}

    right = lax.rem(ring + 1, ring_size)
    left = lax.rem(ring + ring_size - 1, ring_size)

    barrier = pltpu.get_barrier_semaphore()
    peers = [at(ring, lax.rem(me + i, n)) for i in range(1, n)]
    peers += [at(lax.rem(ring + i, ring_size), me) for i in range(1, ring_size)]
    peers += [at(r, lax.rem(me + i, n)) for i in range(1, n) for r in (left, right)]
    for peer in peers:
        pl.semaphore_signal(barrier, inc=1, device_id=peer, device_id_type=MESH)
    pl.semaphore_wait(barrier, len(peers))

    def neighbour(i, src, dst, to):
        return pltpu.make_async_remote_copy(
            src_ref=src,
            dst_ref=dst,
            send_sem=nb_send.at[i],
            recv_sem=nb_recv.at[i],
            device_id=at(to, me),
            device_id_type=MESH,
        )

    near = [
        neighbour(0, payoff_ref.at[rows - SUB : rows], pay.at[0:SUB], right),
        neighbour(1, payoff_ref.at[0:SUB], pay.at[SUB + rows : SUB + rows + SUB], left),
        neighbour(2, offsets_ref, offs.at[0], right),
        neighbour(3, offsets_ref, offs.at[1], left),
    ]
    for copy in near:
        copy.start()

    last = chunks + 1

    def piece(kind, q):
        if kind == 0:
            source = slice((q + 1) * quarter - 1, (q + 1) * quarter)
            target = (q + 1) % n
            return target, (right if q == n - 1 else ring), source, slice(SUB - 1, SUB)
        if kind == last:
            source = slice(q * quarter, q * quarter + 1)
            target = (q - 1) % n
            landing = slice(SUB + quarter, SUB + quarter + 1)
            return target, (left if q == 0 else ring), source, landing
        lo = 0 if kind == 1 else (kind - 1) * span + SUB
        hi = quarter if kind == chunks else kind * span + SUB
        source = slice(q * quarter + lo, q * quarter + hi)
        return q, ring, source, slice(SUB + lo, SUB + hi)

    def table_copy(kind, q):
        target, at_ring, source, landing = piece(kind, q)
        crosses = (kind == 0 and q == n - 1) or (kind == last and q == 0)
        src = tables_ref.at[:, source]
        dst = tab.at[me, :, landing]

        def remote():
            return pltpu.make_async_remote_copy(
                src_ref=src,
                dst_ref=dst,
                send_sem=tab_send.at[kind, q],
                recv_sem=tab_recv.at[kind, me],
                device_id=at(at_ring, target),
                device_id_type=MESH,
            )

        def local():
            return pltpu.make_async_copy(src, dst, tab_recv.at[kind, me])

        return target, crosses, remote, local

    for kind in range(last + 1):
        for q in range(n):
            target, crosses, remote, local = table_copy(kind, q)
            if crosses:
                remote().start()
            else:
                pl.when(me != target)(lambda: remote().start())
                pl.when(me == target)(lambda: local().start())

    own = pltpu.make_async_copy(payoff_ref, pay.at[SUB : SUB + rows], own_sem)
    own.start()
    for copy in near:
        copy.wait()
    own.wait()

    blocks = offsets_ref.shape[1]
    rows_per_block = block_len // LANES
    row_at = lax.broadcasted_iota(jnp.int32, (ext, blocks), 0) + me * quarter
    row_at = row_at + (rows - SUB)
    block_at = row_at // rows_per_block - blocks
    lane_at = lax.broadcasted_iota(jnp.int32, (ext, blocks), 1)
    for s in range(steps):
        def spread(line, shift):
            hit = lane_at == block_at + shift
            return jnp.where(hit, line.astype(jnp.float32), 0.0)

        picked = (
            spread(offsets_ref[s : s + 1, :], 0)
            + spread(offs[0, s : s + 1, :], blocks)
            + spread(offs[1, s : s + 1, :], -blocks)
        )
        branch = jnp.sum(picked, axis=1, keepdims=True)
        kmask[s] = jnp.broadcast_to(branch, (ext, LANES))

    lane = lax.broadcasted_iota(jnp.int32, (wide, LANES), 1)

    def waits(kind, src):
        _, _, source, landing = piece(kind, 0)
        dst = tab.at[src, :, landing]
        pltpu.make_async_copy(tables_ref.at[:, source], dst, tab_recv.at[kind, src]).wait()

    def shifts(x):
        f1 = pltpu.roll(x, LANES - 1, 1)
        f2 = pltpu.roll(x, LANES - 2, 1)
        b1 = pltpu.roll(x, 1, 1)
        b2 = pltpu.roll(x, 2, 1)
        f1 = jnp.where(lane >= LANES - 1, pltpu.roll(f1, wide - 1, 0), f1)
        f2 = jnp.where(lane >= LANES - 2, pltpu.roll(f2, wide - 1, 0), f2)
        b1 = jnp.where(lane < 1, pltpu.roll(b1, 1, 0), b1)
        b2 = jnp.where(lane < 2, pltpu.roll(b2, 1, 0), b2)
        return b2, b1, f1, f2

    def roll_back(h):
        window = slice(h * span, h * span + wide)
        state[0] = pay[pl.ds(pl.multiple_of(me * quarter + h * span, SUB), wide), :]
        for s in reversed(range(steps)):
            src, step = s // per, s % per
            if step == per - 1:
                if h == 0:
                    waits(0, src)
                waits(h + 1, src)
                if h == chunks - 1:
                    waits(last, src)
            w = vol_ref[s] * vol_ref[s]
            discount = tab[src, 0, window, step, :]
            slope_up = discount * tab[src, 2, window, step, :]
            slope_down = discount * tab[src, 4, window, step, :]
            up = discount * tab[src, 1, window, step, :] + w * slope_up
            down = discount * tab[src, 3, window, step, :] + w * slope_down
            middle = discount - up - down
            branch = kmask[s, window]
            low = branch < -0.5
            high = branch > 0.5
            for g in [0] + list(range(s + 2, steps + 1)):
                x = state[g]
                b2, b1, f1, f2 = shifts(x)
                above = jnp.where(low, x, jnp.where(high, f2, f1))
                level = jnp.where(low, b1, jnp.where(high, f1, x))
                below = jnp.where(low, b2, jnp.where(high, x, b1))
                state[g] = up * above + middle * level + down * below
                if g == 0:
                    state[s + 1] = slope_up * (above - level) + slope_down * (below - level)
        here = pl.ds(pl.multiple_of(me * quarter + h * span, SUB), span)
        weights = positions_ref[here, :]
        for g in range(steps + 1):
            center = state[g, SUB : SUB + span, :]
            rows_ref[g, here, :] = center
            if g:
                weighted = jnp.sum(weights * center, axis=0, keepdims=True)
                if h:
                    weighted = weighted + part2[me, g - 1 : g, :]
                part2[me, g - 1 : g, :] = weighted

    def result(m, d, slot, h):
        first = jnp.bitwise_xor(me, m) * quarter + h * span
        held = pl.ds(pl.multiple_of(first, SUB), span)
        return pltpu.make_async_remote_copy(
            src_ref=rows_ref.at[:, held, :],
            dst_ref=rows_ref.at[:, held, :],
            send_sem=res_send.at[slot, h],
            recv_sem=res_recv.at[slot, h],
            device_id=at(ring, jnp.bitwise_xor(me, d)),
            device_id_type=MESH,
        )

    plan = []
    masks = [0]
    d = n // 2
    while d:
        plan += [(m, d) for m in masks]
        masks = masks + [m | d for m in masks]
        d //= 2
    slots = {m | d: i for i, (m, d) in enumerate(plan)}
    landed = set()
    copies = [[result(m, d, i, h) for h in range(chunks)] for i, (m, d) in enumerate(plan)]
    grp_copies = []
    for i in range(1, n):
        grp_copies.append(
            pltpu.make_async_remote_copy(
                src_ref=part2.at[me],
                dst_ref=part2.at[me],
                send_sem=grp_send.at[i],
                recv_sem=grp_recv.at[i],
                device_id=at(ring, lax.rem(me + i, n)),
                device_id_type=MESH,
            )
        )
    ring_copies = []
    for i in range(1, ring_size):
        ring_copies.append(
            pltpu.make_async_remote_copy(
                src_ref=part.at[ring],
                dst_ref=part.at[ring],
                send_sem=ring_send.at[i],
                recv_sem=ring_recv.at[i],
                device_id=at(lax.rem(ring + i, ring_size), me),
                device_id_type=MESH,
            )
        )

    def forward(h):
        for i, (m, d) in enumerate(plan):
            if m != 0:
                if (m, h) not in landed:
                    landed.add((m, h))
                    copies[slots[m]][h].wait_recv()
                copies[i][h].start()

    for h in range(chunks):
        roll_back(h)
        if h == chunks - 1:
            for copy in grp_copies:
                copy.start()
        for i, (m, d) in enumerate(plan):
            if m == 0:
                copies[i][h].start()
    for i in range(1, n):
        src = lax.rem(me + n - i, n)
        pltpu.make_async_copy(part2.at[src], part2.at[src], grp_recv.at[i]).wait()
    part[ring] = jnp.sum(part2[...], axis=0)
    for copy in ring_copies:
        copy.start()
    for h in range(chunks):
        forward(h)
    for i in range(1, ring_size):
        src = lax.rem(ring + ring_size - i, ring_size)
        pltpu.make_async_copy(part.at[src], part.at[src], ring_recv.at[i]).wait()
    sums_ref[...] = jnp.sum(part[...], axis=0)
    for copy in grp_copies + ring_copies:
        copy.wait_send()
    for h in range(chunks):
        for i, (m, d) in enumerate(plan):
            copies[i][h].wait_send()
            if (m | d, h) not in landed:
                copies[i][h].wait_recv()
    for kind in range(last + 1):
        for q in range(n):
            target, crosses, remote, _ = table_copy(kind, q)
            if crosses:
                remote().wait_send()
            else:
                pl.when(me != target)(lambda: remote().wait_send())


def spread_kernel(vol_ref, bucket_ref, bump_ref, rows_ref, sums_ref, out_ref, vega_ref):
    curves = bucket_ref.shape[0]
    base = rows_ref[0]
    for b in range(curves):
        s = bucket_ref[b]
        change = bump_ref[b] * (2.0 * vol_ref[s] + bump_ref[b])
        out_ref[b // SUB, :, b % SUB, :] = base + change * rows_ref[s + 1]

    @pl.when(pl.program_id(0) == 0)
    def _():
        lane = lax.broadcasted_iota(jnp.int32, (1, curves), 1)
        total = jnp.zeros((1, curves), jnp.float32)
        for b in range(curves):
            s = bucket_ref[b]
            slope = 2.0 * vol_ref[s] + bump_ref[b]
            weighted = jnp.sum(sums_ref[pl.ds(s, 1), :], axis=1, keepdims=True)
            total = jnp.where(lane == b, slope * weighted, total)
        vega_ref[...] = total


def on_device(n, nx, ny, payoff, positions, tables, offsets, vol_curve, bucket, bump_size):
    steps = vol_curve.shape[0]
    per, comps, nodes = tables.shape
    curves = bucket.shape[0]
    rows = nodes // LANES
    block_len = nodes // offsets.shape[1]
    quarter = rows // n
    ext = quarter + 2 * SUB
    ring = nx * ny
    chunks = 2
    wide = quarter // chunks + 2 * SUB
    tiles = tables.transpose(1, 0, 2).reshape(comps, per, rows, LANES).transpose(0, 2, 1, 3)
    dma = pltpu.SemaphoreType.DMA
    vmem = pl.BlockSpec(memory_space=pltpu.VMEM)
    smem = pl.BlockSpec(memory_space=pltpu.SMEM)
    moved, sums = pl.pallas_call(
        functools.partial(sweep_kernel, (n, nx, ny, steps, per, block_len, chunks)),
        out_shape=(
            jax.ShapeDtypeStruct((steps + 1, rows, LANES), jnp.float32),
            jax.ShapeDtypeStruct((steps, LANES), jnp.float32),
        ),
        in_specs=[smem, vmem, vmem, vmem, pl.BlockSpec(memory_space=pl.ANY)],
        out_specs=(vmem, vmem),
        scratch_shapes=[
            pltpu.VMEM((n, comps, ext, per, LANES), jnp.float32),
            pltpu.VMEM((rows + 2 * SUB, LANES), jnp.float32),
            pltpu.VMEM((2,) + offsets.shape, jnp.int32),
            pltpu.VMEM((steps, ext, LANES), jnp.float32),
            pltpu.VMEM((steps + 1, wide, LANES), jnp.float32),
            pltpu.VMEM((ring, steps, LANES), jnp.float32),
            pltpu.VMEM((n, steps, LANES), jnp.float32),
            dma((chunks + 2, n)),
            dma((chunks + 2, n)),
            dma((4,)),
            dma((4,)),
            dma,
            dma((n - 1, chunks)),
            dma((n - 1, chunks)),
            dma((ring,)),
            dma((ring,)),
            dma((n,)),
            dma((n,)),
        ],
        compiler_params=pltpu.CompilerParams(has_side_effects=True, collective_id=0),
        name="sweep",
    )(
        vol_curve,
        payoff.reshape(rows, LANES),
        positions.reshape(rows, LANES),
        offsets,
        tiles,
    )
    grid = max(1, n // 2)
    groups = curves // SUB
    bumped, vega = pl.pallas_call(
        spread_kernel,
        grid=(grid,),
        out_shape=(
            jax.ShapeDtypeStruct((groups, rows, SUB, LANES), jnp.float32),
            jax.ShapeDtypeStruct((1, curves), jnp.float32),
        ),
        in_specs=[
            smem,
            smem,
            smem,
            pl.BlockSpec((steps + 1, rows // grid, LANES), lambda i: (0, i, 0)),
            pl.BlockSpec((steps, LANES), lambda i: (0, 0)),
        ],
        out_specs=(
            pl.BlockSpec((groups, rows // grid, SUB, LANES), lambda i: (0, i, 0, 0)),
            pl.BlockSpec((1, curves), lambda i: (0, 0)),
        ),
        name="spread",
    )(vol_curve, bucket, bump_size, moved, sums)
    bumped = bumped.transpose(0, 2, 1, 3).reshape(curves, nodes)
    return bumped, vega.reshape(curves)


def solution(mesh):
    shape = dict(mesh.shape)
    in_specs = (
        P(("nx", "ny")),
        P(("nx", "ny")),
        P("bump", None, ("nx", "ny")),
        P(None, ("nx", "ny")),
        P(),
        P("bump"),
        P("bump"),
    )
    out_specs = (P("bump", ("nx", "ny")), P("bump"))
    body = functools.partial(on_device, shape["bump"], shape["nx"], shape["ny"])
    return jax.shard_map(body, mesh=mesh, in_specs=in_specs, out_specs=out_specs, check_vma=False)
```
